32 devices in a mesh: south: 4 (over z), east: 4 (over y, x), down: 2 (over core).
Axes of the slice: x: 2, y: 2, z: 4, core: 2. Of those that a mesh axis runs over, the one named last changes fastest.
Arguments:
- initial_scalar_state: float32 [16, 128, 256, 128], P('south', 'east', 'down'), may hold values from 0.2 to 1.8
- scaled_wind_second: float32 [16, 128, 256, 128], P('south', 'east', 'down'), may hold values from -0.3 to 0.3
- scaled_wind_first: float32 [16, 128, 256, 128], P('south', 'east', 'down'), may hold values from -0.3 to 0.3
- scaled_wind_third: float32 [16, 128, 256, 128], P('south', 'east', 'down'), may hold values from -0.3 to 0.3
Outputs:
- temperature_end: float32 [16, 128, 256, 128], P('south', 'east', 'down')
The draws below stay inside these ranges and needn't reach their ends.
All inputs are finite; a program needn't handle non-finite values.
Results may differ from the reference program's by a relative error of at most 0.00002.
Values sent between devices are 32-bit elements; how exact they have to be, the bound alone decides.
A program may use at most 448 MiB of HBM per device.

```python
import jax
import jax.numpy as jnp
from jax import lax

SECOND_AXIS_SIZE = 16
FIRST_AXIS_SIZE = 128
THIRD_AXIS_SIZE = 256
HEIGHT_COUNT = 128
STEPS = 4


def steps_of(stream_key, extent, split, low, largest):
    gain, own = 1.0, jax.random.fold_in(stream_key, 6)
    for axis_at, shards_of in split:
        steps = jnp.exp(jax.random.uniform(jax.random.fold_in(own, axis_at), (shards_of,), jnp.float32, low / len(split), largest / len(split)))
        gain = gain * jnp.repeat(steps, extent[axis_at] // shards_of).reshape([-1 if axis == axis_at else 1 for axis in range(len(extent))])
    return gain


def setup_inputs(seed: int = 0) -> dict:
    arg_keys = jax.random.split(jax.random.key(seed), 5)
    initial_scalar_state = jnp.clip(0.2 + 1.5999999 * jax.random.uniform(arg_keys[0], (SECOND_AXIS_SIZE, FIRST_AXIS_SIZE, THIRD_AXIS_SIZE, HEIGHT_COUNT), jnp.float32) ** steps_of(arg_keys[0], (SECOND_AXIS_SIZE, FIRST_AXIS_SIZE, THIRD_AXIS_SIZE, HEIGHT_COUNT), ((0, 4), (1, 4), (2, 2)), -0.2, 0.2), 0.2, 1.8)
    scaled_wind_second = jnp.clip(jax.random.uniform(arg_keys[1], (SECOND_AXIS_SIZE, FIRST_AXIS_SIZE, THIRD_AXIS_SIZE, HEIGHT_COUNT), jnp.float32, -0.3, 0.3) * steps_of(arg_keys[1], (SECOND_AXIS_SIZE, FIRST_AXIS_SIZE, THIRD_AXIS_SIZE, HEIGHT_COUNT), ((0, 4), (1, 4), (2, 2)), -0.4, 0.0), -0.3, 0.3)
    scaled_wind_first = jnp.clip(jax.random.uniform(arg_keys[2], (SECOND_AXIS_SIZE, FIRST_AXIS_SIZE, THIRD_AXIS_SIZE, HEIGHT_COUNT), jnp.float32, -0.3, 0.3) * steps_of(arg_keys[2], (SECOND_AXIS_SIZE, FIRST_AXIS_SIZE, THIRD_AXIS_SIZE, HEIGHT_COUNT), ((0, 4), (1, 4), (2, 2)), -0.4, 0.0), -0.3, 0.3)
    scaled_wind_third = jnp.clip(jax.random.uniform(arg_keys[3], (SECOND_AXIS_SIZE, FIRST_AXIS_SIZE, THIRD_AXIS_SIZE, HEIGHT_COUNT), jnp.float32, -0.3, 0.3) * steps_of(arg_keys[3], (SECOND_AXIS_SIZE, FIRST_AXIS_SIZE, THIRD_AXIS_SIZE, HEIGHT_COUNT), ((0, 4), (1, 4), (2, 2)), -0.4, 0.0), -0.3, 0.3)
    return {"initial_scalar_state": initial_scalar_state, "scaled_wind_second": scaled_wind_second, "scaled_wind_first": scaled_wind_first, "scaled_wind_third": scaled_wind_third}


def strip_edges(values, dims):
    for dim in dims:
        values = lax.slice_in_dim(values, 1, values.shape[dim] - 1, axis=dim)
    return values


def neighbour(values, dim, start, dims):
    others = [other for other in dims if other != dim]
    values = strip_edges(values, others)
    return lax.slice_in_dim(values, start, start + values.shape[dim] - 2, axis=dim)


def update_lone_timestep(padded_with_margin, scaled_wind_second, scaled_wind_first, scaled_wind_third):
    middle = strip_edges(padded_with_margin, (0, 1, 2))
    lower = [neighbour(padded_with_margin, dim, 0, (0, 1, 2)) for dim in (0, 1, 2)]
    upper = [neighbour(padded_with_margin, dim, 2, (0, 1, 2)) for dim in (0, 1, 2)]
    slopes = [above - below for above, below in zip(upper, lower)]
    smooth_rate = 0.05
    spread = lower[0] + upper[0] + lower[1] + upper[1] + lower[2] + upper[2] - 6.0 * middle
    return middle - scaled_wind_second * slopes[0] - scaled_wind_first * slopes[1] - scaled_wind_third * slopes[2] + smooth_rate * spread


def reference(initial_scalar_state, scaled_wind_second, scaled_wind_first, scaled_wind_third):
    for step in range(STEPS):
        initial_scalar_state = update_lone_timestep(jnp.pad(initial_scalar_state, ((1, 1), (1, 1), (1, 1), (0, 0)), mode="wrap"), scaled_wind_second, scaled_wind_first, scaled_wind_third)
    return initial_scalar_state
```

```python
import functools

import jax
import jax.numpy as jnp
from jax import lax
from jax.experimental import pallas as pl
from jax.experimental.pallas import tpu as pltpu
from jax.sharding import PartitionSpec as P

STEPS = 4
CHUNKS = 8
TILE = 8
MESH = pl.DeviceIdType.MESH


def beside(axis, shift):
    size = lax.axis_size(axis)
    return {axis: lax.rem(lax.axis_index(axis) + size + shift, size)}


def kernel(
    x, wind_j, wind_i, wind_k, out, state, winds, x_sem, wind_sem, out_sem,
    j_send, j_recv, i_send, i_recv, k_send, k_recv,
):
    J, I, K, _ = x.shape
    width = I // CHUNKS
    inner = pl.ds(TILE, K)
    winds_in = (wind_j, wind_i, wind_k)

    def j_copy(way, step, chunk, first):
        slot, row = lax.rem(step, 2), chunk * width
        if first:
            src = x.at[(J - 1, 0)[way], pl.ds(row, width)]
        else:
            src = state.at[slot, (J, 1)[way], pl.ds(row + 1, width), inner]
        return pltpu.make_async_remote_copy(
            src_ref=src,
            dst_ref=state.at[slot, (0, J + 1)[way], pl.ds(row + 1, width), inner],
            send_sem=j_send.at[way, step, chunk],
            recv_sem=j_recv.at[way, step, chunk],
            device_id=beside("south", (1, -1)[way]),
            device_id_type=MESH,
        )

    def i_copy(way, step, first):
        slot = lax.rem(step, 2)
        if first:
            src = x.at[:, (I - 1, 0)[way]]
        else:
            src = state.at[slot, pl.ds(1, J), (I, 1)[way], inner]
        return pltpu.make_async_remote_copy(
            src_ref=src,
            dst_ref=state.at[slot, pl.ds(1, J), (0, I + 1)[way], inner],
            send_sem=i_send.at[way, step],
            recv_sem=i_recv.at[way, step],
            device_id=beside("east", (1, -1)[way]),
            device_id_type=MESH,
        )

    def k_copy(way, step, chunk, first):
        slot, row = lax.rem(step, 2), chunk * width
        if first:
            src = x.at[:, pl.ds(row, width), pl.ds((K - TILE, 0)[way], TILE)]
        else:
            src = state.at[
                slot, pl.ds(1, J), pl.ds(row + 1, width), pl.ds((K, TILE)[way], TILE)
            ]
        return pltpu.make_async_remote_copy(
            src_ref=src,
            dst_ref=state.at[
                slot, pl.ds(1, J), pl.ds(row + 1, width), pl.ds((0, K + TILE)[way], TILE)
            ],
            send_sem=k_send.at[way, step, chunk],
            recv_sem=k_recv.at[way, step, chunk],
            device_id=beside("down", (1, -1)[way]),
            device_id_type=MESH,
        )

    def x_copy(chunk):
        rows = pl.ds(chunk * width, width)
        return pltpu.make_async_copy(
            x.at[:, rows],
            state.at[0, pl.ds(1, J), pl.ds(chunk * width + 1, width), inner],
            x_sem.at[chunk],
        )

    def wind_copy(which, chunk):
        rows = pl.ds(chunk * width, width)
        return pltpu.make_async_copy(
            winds_in[which].at[:, rows], winds.at[which, :, rows], wind_sem.at[which, chunk]
        )

    def out_copy(chunk):
        rows = pl.ds(chunk * width, width)
        return pltpu.make_async_copy(
            state.at[STEPS % 2, pl.ds(1, J), pl.ds(chunk * width + 1, width), inner],
            out.at[:, rows],
            out_sem.at[chunk],
        )

    def chunk_at(place):
        return jnp.where(lax.rem(place, 2) == 0, place // 2, CHUNKS - 1 - place // 2)

    def send(step, chunk, first):
        for way in (0, 1):
            j_copy(way, step, chunk, first).start()
        for way in (0, 1):
            @pl.when(chunk == (CHUNKS - 1, 0)[way])
            def _():
                i_copy(way, step, first).start()
        for way in (0, 1):
            k_copy(way, step, chunk, first).start()

    def wait_sent(step, chunk, first):
        for way in (0, 1):
            j_copy(way, step, chunk, first).wait_send()
            k_copy(way, step, chunk, first).wait_send()

            @pl.when(chunk == (CHUNKS - 1, 0)[way])
            def _():
                i_copy(way, step, first).wait_send()

    def wait_received(step, chunk):
        for way in (0, 1):
            k_copy(way, step, chunk, False).wait_recv()

            @pl.when(chunk == (0, CHUNKS - 1)[way])
            def _():
                i_copy(way, step, False).wait_recv()

            j_copy(way, step, chunk, False).wait_recv()

    def update(step, chunk):
        now = lax.rem(step, 2)
        later = 1 - now

        def one_row(n, _):
            i = chunk * width + n
            for j in range(1, J + 1):
                middle = state[now, j, i + 1, inner, :]
                j_low, j_high = state[now, j - 1, i + 1, inner, :], state[now, j + 1, i + 1, inner, :]
                i_low, i_high = state[now, j, i, inner, :], state[now, j, i + 2, inner, :]
                k_low = state[now, j, i + 1, pl.ds(TILE - 1, K), :]
                k_high = state[now, j, i + 1, pl.ds(TILE + 1, K), :]
                spread = j_low + j_high + i_low + i_high + k_low + k_high - 6.0 * middle
                state[later, j, i + 1, inner, :] = (
                    middle
                    - winds[0, j - 1, i] * (j_high - j_low)
                    - winds[1, j - 1, i] * (i_high - i_low)
                    - winds[2, j - 1, i] * (k_high - k_low)
                    + 0.05 * spread
                )
            return 0

        lax.fori_loop(0, width, one_row, 0)

    def over(body):
        def one(place, _):
            body(chunk_at(place))
            return 0

        lax.fori_loop(0, CHUNKS, one, 0)

    barrier = pltpu.get_barrier_semaphore()
    for axis in ("south", "east", "down"):
        for shift in (1, -1):
            pl.semaphore_signal(
                barrier, inc=1, device_id=beside(axis, shift), device_id_type=MESH
            )
    over(lambda chunk: x_copy(chunk).start())
    pl.semaphore_wait(barrier, 6)
    over(lambda chunk: send(0, chunk, True))

    def load_winds(chunk):
        for which in range(3):
            wind_copy(which, chunk).start()

    over(load_winds)
    over(lambda chunk: x_copy(chunk).wait())

    def one_step(step, _):
        def one_chunk(chunk):
            @pl.when(step == 0)
            def _():
                for which in range(3):
                    wind_copy(which, chunk).wait()

            @pl.when(step == 1)
            def _():
                wait_sent(0, chunk, True)

            @pl.when(step > 1)
            def _():
                wait_sent(step - 1, chunk, False)

            wait_received(step, chunk)
            update(step, chunk)

            @pl.when(step < STEPS - 1)
            def _():
                send(step + 1, chunk, False)

            @pl.when(step == STEPS - 1)
            def _():
                out_copy(chunk).start()

        over(one_chunk)
        return 0

    lax.fori_loop(0, STEPS, one_step, 0)
    over(lambda chunk: wait_sent(STEPS - 1, chunk, False))
    over(lambda chunk: out_copy(chunk).wait())


def on_device(x, wind_j, wind_i, wind_k):
    J, I, K, L = x.shape
    dma = pltpu.SemaphoreType.DMA
    return pl.pallas_call(
        kernel,
        out_shape=jax.ShapeDtypeStruct(x.shape, x.dtype),
        in_specs=[pl.BlockSpec(memory_space=pl.ANY)] * 4,
        out_specs=pl.BlockSpec(memory_space=pl.ANY),
        scratch_shapes=[
            pltpu.VMEM((2, J + 2, I + 2, K + 2 * TILE, L), x.dtype),
            pltpu.VMEM((3, J, I, K, L), x.dtype),
            dma((CHUNKS,)),
            dma((3, CHUNKS)),
            dma((CHUNKS,)),
            dma((2, STEPS, CHUNKS)),
            dma((2, STEPS, CHUNKS)),
            dma((2, STEPS)),
            dma((2, STEPS)),
            dma((2, STEPS, CHUNKS)),
            dma((2, STEPS, CHUNKS)),
        ],
        compiler_params=pltpu.CompilerParams(
            collective_id=0, has_side_effects=True, vmem_limit_bytes=67043328
        ),
    )(x, wind_j, wind_i, wind_k)


def solution(mesh):
    placed = P("south", "east", "down", None)
    return jax.shard_map(
        on_device, mesh=mesh, in_specs=(placed,) * 4, out_specs=placed, check_vma=False
    )
```

```python
import functools

import jax
import jax.numpy as jnp
from jax import lax
from jax.experimental import pallas as pl
from jax.experimental.pallas import tpu as pltpu
from jax.sharding import PartitionSpec as P

STEPS = 4
CHUNKS = 4
TILE = 8
MESH = pl.DeviceIdType.MESH


def beside(axis, shift):
    size = lax.axis_size(axis)
    return {axis: lax.rem(lax.axis_index(axis) + size + shift, size)}


def kernel(
    x, wind_j, wind_i, wind_k, out, state, winds, x_sem, wind_sem,
    j_send, j_recv, i_send, i_recv, k_send, k_recv,
):
    J, I, K, _ = x.shape
    width = I // CHUNKS
    inner = pl.ds(TILE, K)
    winds_in = (wind_j, wind_i, wind_k)

    def j_copy(way, step, chunk, first):
        slot, row = lax.rem(step, 2), chunk * width
        if first:
            src = x.at[(J - 1, 0)[way], pl.ds(row, width)]
        else:
            src = state.at[slot, (J, 1)[way], pl.ds(row + 1, width), inner]
        return pltpu.make_async_remote_copy(
            src_ref=src,
            dst_ref=state.at[slot, (0, J + 1)[way], pl.ds(row + 1, width), inner],
            send_sem=j_send.at[way, step, chunk],
            recv_sem=j_recv.at[way, step, chunk],
            device_id=beside("south", (1, -1)[way]),
            device_id_type=MESH,
        )

    def i_copy(way, step, first):
        slot = lax.rem(step, 2)
        if first:
            src = x.at[:, (I - 1, 0)[way]]
        else:
            src = state.at[slot, pl.ds(1, J), (I, 1)[way], inner]
        return pltpu.make_async_remote_copy(
            src_ref=src,
            dst_ref=state.at[slot, pl.ds(1, J), (0, I + 1)[way], inner],
            send_sem=i_send.at[way, step],
            recv_sem=i_recv.at[way, step],
            device_id=beside("east", (1, -1)[way]),
            device_id_type=MESH,
        )

    def k_copy(way, step, chunk, first):
        slot, row = lax.rem(step, 2), chunk * width
        if first:
            src = x.at[:, pl.ds(row, width), pl.ds((K - TILE, 0)[way], TILE)]
        else:
            src = state.at[
                slot, pl.ds(1, J), pl.ds(row + 1, width), pl.ds((K, TILE)[way], TILE)
            ]
        return pltpu.make_async_remote_copy(
            src_ref=src,
            dst_ref=state.at[
                slot, pl.ds(1, J), pl.ds(row + 1, width), pl.ds((0, K + TILE)[way], TILE)
            ],
            send_sem=k_send.at[way, step, chunk],
            recv_sem=k_recv.at[way, step, chunk],
            device_id=beside("down", (1, -1)[way]),
            device_id_type=MESH,
        )

    def x_copy(chunk):
        rows = pl.ds(chunk * width, width)
        return pltpu.make_async_copy(
            x.at[:, rows],
            state.at[0, pl.ds(1, J), pl.ds(chunk * width + 1, width), inner],
            x_sem.at[chunk],
        )

    def wind_copy(which, chunk):
        rows = pl.ds(chunk * width, width)
        return pltpu.make_async_copy(
            winds_in[which].at[:, rows], winds.at[which, :, rows], wind_sem.at[which, chunk]
        )

    def chunk_at(place):
        return jnp.where(lax.rem(place, 2) == 0, place // 2, CHUNKS - 1 - place // 2)

    def send(step, chunk, first):
        for way in (0, 1):
            j_copy(way, step, chunk, first).start()
        for way in (0, 1):
            @pl.when(chunk == (CHUNKS - 1, 0)[way])
            def _():
                i_copy(way, step, first).start()
        for way in (0, 1):
            k_copy(way, step, chunk, first).start()

    def wait_sent(step, chunk, first):
        for way in (0, 1):
            j_copy(way, step, chunk, first).wait_send()
            k_copy(way, step, chunk, first).wait_send()

            @pl.when(chunk == (CHUNKS - 1, 0)[way])
            def _():
                i_copy(way, step, first).wait_send()

    def wait_received(step, chunk):
        for way in (0, 1):
            k_copy(way, step, chunk, False).wait_recv()

            @pl.when(chunk == (0, CHUNKS - 1)[way])
            def _():
                i_copy(way, step, False).wait_recv()

            j_copy(way, step, chunk, False).wait_recv()

    def update(step, chunk, store):
        now = lax.rem(step, 2)

        def one_row(n, _):
            i = chunk * width + n
            for j in range(1, J + 1):
                middle = state[now, j, i + 1, inner, :]
                j_low, j_high = state[now, j - 1, i + 1, inner, :], state[now, j + 1, i + 1, inner, :]
                i_low, i_high = state[now, j, i, inner, :], state[now, j, i + 2, inner, :]
                k_low = state[now, j, i + 1, pl.ds(TILE - 1, K), :]
                k_high = state[now, j, i + 1, pl.ds(TILE + 1, K), :]
                spread = j_low + j_high + i_low + i_high + k_low + k_high - 6.0 * middle
                store(
                    j,
                    i,
                    middle
                    - winds[0, j - 1, i] * (j_high - j_low)
                    - winds[1, j - 1, i] * (i_high - i_low)
                    - winds[2, j - 1, i] * (k_high - k_low)
                    + 0.05 * spread,
                )
            return 0

        lax.fori_loop(0, width, one_row, 0)

    def over(body):
        def one(place, _):
            body(chunk_at(place))
            return 0

        lax.fori_loop(0, CHUNKS, one, 0)

    barrier = pltpu.get_barrier_semaphore()
    for axis in ("south", "east", "down"):
        for shift in (1, -1):
            pl.semaphore_signal(
                barrier, inc=1, device_id=beside(axis, shift), device_id_type=MESH
            )
    over(lambda chunk: x_copy(chunk).start())
    pl.semaphore_wait(barrier, 6)
    over(lambda chunk: send(0, chunk, True))

    def load_winds(chunk):
        for which in range(3):
            wind_copy(which, chunk).start()

    over(load_winds)
    over(lambda chunk: x_copy(chunk).wait())

    def one_step(step, _):
        def one_chunk(chunk):
            @pl.when(step == 0)
            def _():
                for which in range(3):
                    wind_copy(which, chunk).wait()

            @pl.when(step == 1)
            def _():
                wait_sent(0, chunk, True)

            @pl.when(step > 1)
            def _():
                wait_sent(step - 1, chunk, False)

            wait_received(step, chunk)

            @pl.when(step < STEPS - 1)
            def _():
                def keep(j, i, values):
                    state[1 - lax.rem(step, 2), j, i + 1, inner, :] = values

                update(step, chunk, keep)
                send(step + 1, chunk, False)

            @pl.when(step == STEPS - 1)
            def _():
                def give(j, i, values):
                    out[j - 1, i] = values

                update(step, chunk, give)

        over(one_chunk)
        return 0

    lax.fori_loop(0, STEPS, one_step, 0)
    over(lambda chunk: wait_sent(STEPS - 1, chunk, False))


def on_device(x, wind_j, wind_i, wind_k):
    J, I, K, L = x.shape
    dma = pltpu.SemaphoreType.DMA
    return pl.pallas_call(
        kernel,
        out_shape=pltpu.VMEM(x.shape, x.dtype),
        in_specs=[pl.BlockSpec(memory_space=pl.ANY)] * 4,
        out_specs=pl.BlockSpec(memory_space=pltpu.VMEM),
        scratch_shapes=[
            pltpu.VMEM((2, J + 2, I + 2, K + 2 * TILE, L), x.dtype),
            pltpu.VMEM((3, J, I, K, L), x.dtype),
            dma((CHUNKS,)),
            dma((3, CHUNKS)),
            dma((2, STEPS, CHUNKS)),
            dma((2, STEPS, CHUNKS)),
            dma((2, STEPS)),
            dma((2, STEPS)),
            dma((2, STEPS, CHUNKS)),
            dma((2, STEPS, CHUNKS)),
        ],
        compiler_params=pltpu.CompilerParams(
            collective_id=0, has_side_effects=True, vmem_limit_bytes=54 * 2**20
        ),
    )(x, wind_j, wind_i, wind_k)


def solution(mesh):
    placed = P("south", "east", "down", None)
    return jax.shard_map(
        on_device, mesh=mesh, in_specs=(placed,) * 4, out_specs=placed, check_vma=False
    )
```
